32 devices in a mesh: rows: 8 (over z, x), cols: 4 (over y, core).
Axes of the slice: x: 2, y: 2, z: 4, core: 2. Of those that a mesh axis runs over, the one named last changes fastest.
Arguments:
- matrix: float32 [512, 32, 2, 128], P('rows', 'cols'), may hold values from -54 to 54
- plan: int32 [2, 4, 256], replicated, may hold values from 0 to 255, as said below
Outputs:
- rotated: float32 [512, 32, 2, 128], P('rows', 'cols')
The draws below stay inside these ranges and needn't reach their ends.
Inputs may be any that keep to these rules, and one draw needn't show every extreme that they name: Each plan[s, r] pairs the 256 columns: partner of partner of i is i, and no column is its own partner.
All inputs are finite; a program needn't handle non-finite values.
Results may differ from the reference program's by a relative error of at most 0.0003.
Values sent between devices are 32-bit elements; how exact they have to be, the bound alone decides.
A program may use at most 128 MiB of HBM per device.

```python
import math
import jax
import jax.numpy as jnp
from jax import lax

BLOCK = 128
PAIR_DEV = 8
STEPS = 2
ROUNDS = 4
PAIRS = 32
ROWS = 512


def draw_matrix(key, part):
    base_key = jax.random.fold_in(key, 11)
    first, second, third = jax.random.split(base_key, 3)
    shape = (ROWS, PAIRS, 2, BLOCK)
    row_scale = jnp.exp(jax.random.uniform(second, (ROWS, 1, 1, 1), jnp.float32, math.log(0.3), math.log(3.0)))
    col_scale = jnp.exp(jax.random.uniform(third, (1, PAIRS, 2, BLOCK), jnp.float32, math.log(0.3), math.log(3.0)))
    values = jnp.clip(jax.random.normal(first, shape, jnp.float32), -6.0, 6.0)
    return (values * row_scale * col_scale).astype(jnp.float32)


def draw_plan(key, part):
    width = 2 * BLOCK

    def one_table(inner_key):
        order = jax.random.permutation(inner_key, width).astype(jnp.int32)
        first_half = order[0::2]
        second_half = order[1::2]
        partner = jnp.zeros((width,), jnp.int32).at[first_half].set(second_half).at[second_half].set(first_half)
        return partner
    keys = jax.random.split(jax.random.fold_in(key, 7), STEPS * ROUNDS)
    tables = jax.vmap(one_table)(keys)
    return tables.reshape(STEPS, ROUNDS, width).astype(jnp.int32)


def setup_inputs(seed: int = 0) -> dict:
    streams_of = jax.random.split(jax.random.key(seed), 3)
    return {
        "matrix": draw_matrix(jax.random.fold_in(streams_of[2], 71), 0),
        "plan": draw_plan(jax.random.fold_in(streams_of[2], 71), 0),
    }


def diagonalize(grams, table):
    width = grams.shape[1]
    indices = jnp.arange(width, dtype=jnp.int32)
    rotation = jnp.broadcast_to(jnp.eye(width, dtype=jnp.float32), grams.shape)
    unit_matrix = jnp.eye(width, dtype=jnp.float32)
    for round_index in range(table.shape[0]):
        partner = table[round_index]
        onehot = (partner[:, None] == indices[None, :]).astype(jnp.float32)
        diagonal_now = jnp.diagonal(grams, axis1=1, axis2=2)
        partner_diag = jnp.einsum('pj,ij->pi', diagonal_now, onehot, precision=lax.Precision.HIGHEST)
        partner_gram = lax.optimization_barrier(jnp.sum(grams * onehot[None], axis=2))
        orient = jnp.where(indices < partner, 1.0, -1.0).astype(jnp.float32)
        spread = orient[None, :] * (partner_diag - diagonal_now)
        sign_part = jnp.where(spread >= 0.0, 1.0, -1.0).astype(jnp.float32)
        tangent = sign_part * 2.0 * partner_gram / (jnp.abs(spread) + jnp.sqrt(spread * spread + 4.0 * partner_gram * partner_gram))
        cosine = 1.0 / jnp.sqrt(1.0 + tangent * tangent)
        sine_part = tangent * cosine
        off_part = jnp.swapaxes(onehot[None] * (-orient[None, :] * sine_part)[:, :, None], 1, 2)
        rot_now = cosine[:, :, None] * unit_matrix[None] + off_part
        product = jnp.einsum('pij,pjk->pik', grams, rot_now, precision=lax.Precision.HIGHEST)
        grams = jnp.einsum('pji,pjk->pik', rot_now, product, precision=lax.Precision.HIGHEST)
        rotation = jnp.einsum('pij,pjk->pik', rotation, rot_now, precision=lax.Precision.HIGHEST)
    return (grams, rotation)

def reference(matrix, plan):
    rows_all, pairs, halves, width = matrix.shape
    columns = matrix.reshape(rows_all, pairs, halves * width)
    for step_index in range(STEPS):
        grams = jnp.einsum('mpi,mpj->pij', columns, columns, precision=lax.Precision.HIGHEST)
        grams, rotation = diagonalize(grams, plan[step_index])
        columns = jnp.einsum('mpi,pij->mpj', columns, rotation, precision=lax.Precision.HIGHEST)
        quarter = columns.reshape(rows_all, pairs, halves, width)
        tops = quarter[:, :, 0, :]
        bottoms = jnp.roll(quarter[:, :, 1, :], PAIR_DEV, axis=1)
        columns = jnp.stack([tops, bottoms], axis=2).reshape(rows_all, pairs, halves * width)
    return columns.reshape(matrix.shape)
```

```python
import functools

import jax
import jax.numpy as jnp
from jax import lax
from jax.experimental import pallas as pl
from jax.experimental.pallas import tpu as pltpu
from jax.sharding import PartitionSpec as P

MESH = pl.DeviceIdType.MESH
NN = (((1,), (0,)), ((), ()))
NT = (((1,), (1,)), ((), ()))
F32 = jnp.float32
BF16 = jnp.bfloat16


def dot(a, b, dims=NN, precision=None):
    return lax.dot_general(a, b, dims, precision=precision, preferred_element_type=F32)


def exact_dot(a, b, dims=NN):
    return dot(a, b, dims, lax.Precision.HIGHEST)


def split(a):
    hi = a.astype(BF16)
    rest = a - hi.astype(F32)
    mid = rest.astype(BF16)
    lo = (rest - mid.astype(F32)).astype(BF16)
    return hi, mid, lo


def moved_columns(a, onehot):
    hi, mid, lo = split(a)
    return dot(hi, onehot) + dot(mid, onehot) + dot(lo, onehot)


def moved_transposed(a, onehot_t):
    hi, mid, lo = split(a)
    return dot(onehot_t, hi, NT) + dot(onehot_t, mid, NT) + dot(onehot_t, lo, NT)


def rotated_columns(a, cosine, sine):
    half = a.shape[1] // 2
    left, right = a[:, :half], a[:, half:]
    return jnp.concatenate([cosine * left - sine * right, sine * left + cosine * right], axis=1)


def angles(gram):
    half = gram.shape[0] // 2
    shape = (half, half)
    eye = lax.broadcasted_iota(jnp.int32, shape, 0) == lax.broadcasted_iota(jnp.int32, shape, 1)

    def diagonal(block):
        return jnp.sum(jnp.where(eye, block, 0.0), axis=0, keepdims=True)

    low = diagonal(gram[:half, :half])
    high = diagonal(gram[half:, half:])
    cross = diagonal(gram[:half, half:])
    spread = high - low
    sign = jnp.where(spread >= 0.0, 1.0, -1.0)
    root = jnp.sqrt(spread * spread + 4.0 * cross * cross)
    tangent = sign * 2.0 * cross / (jnp.abs(spread) + root)
    cosine = 1.0 / jnp.sqrt(1.0 + tangent * tangent)
    return cosine, tangent * cosine


def orders(partner):
    width = partner.shape[1]
    shape = (width, width)
    row = lax.broadcasted_iota(jnp.int32, shape, 0)
    col = lax.broadcasted_iota(jnp.int32, shape, 1)
    other = jnp.broadcast_to(partner, shape)
    swap = row == other
    one = jnp.ones(shape, BF16)

    def bits(mask):
        return jnp.where(mask, 1.0, 0.0).astype(BF16)

    swap_b = bits(swap)
    first_row = other > col
    rank_row = dot(bits(first_row), bits(row < col))
    mate_row = dot(rank_row.astype(BF16), swap_b)
    place_row = jnp.where(first_row, rank_row, mate_row + float(width // 2))
    first_col = dot(bits(swap & (col > row)), one) > 0.5
    rank_col = dot(bits(col < row), bits(first_col))
    mate_col = dot(swap_b, rank_col.astype(BF16))
    place_col = jnp.where(first_col, rank_col, mate_col + float(width // 2))
    forward = bits(place_col == col.astype(F32))
    backward = bits(place_row == row.astype(F32))
    return forward, backward


def diagonalizer(gram, step, moves, moves_t, rounds):
    rotation = None
    cosine = sine = None
    for r in range(rounds):
        move = moves[step, r]
        if r == 0:
            turned = moved_transposed(gram, moves_t[step, r])
            gram = moved_columns(turned, move)
            rotation = move.astype(F32)
        else:
            turned = moved_transposed(rotated_columns(gram, cosine, sine), moves_t[step, r])
            gram = moved_columns(rotated_columns(turned, cosine, sine), move)
            rotation = moved_columns(rotation, move)
        cosine, sine = angles(gram)
        rotation = rotated_columns(rotation, cosine, sine)
    return moved_columns(rotation, moves[step, rounds])


def kernel(sizes, x_ref, plan_ref, out_ref, stage, held, bottoms, landed, ytop, ybot, arrived, moves, moves_t, grams,
           in_send, in_recv, mid_sem, gram_send, gram_recv, top_send, top_recv, low_send, low_recv):
    owners, groups, cols, rows_here, steps, rounds, width = sizes
    half = width // 2
    rows_all = owners * rows_here
    me = lax.axis_index("rows")
    col = lax.axis_index("cols")
    group, mine = me // owners, me % owners
    right = (col + 1) % cols

    def at(owner_shift, col_shift=0, group_shift=0):
        row = ((group + group_shift) % groups) * owners + (mine + owner_shift) % owners
        return row, (col + col_shift) % cols

    peers = {(o, c, 0) for o in range(owners) for c in (0, 1, cols - 1)} | {(0, 0, g) for g in range(groups)}
    peers = sorted(peers - {(0, 0, 0)})
    barrier = pltpu.get_barrier_semaphore()
    for peer in peers:
        pl.semaphore_signal(barrier, inc=1, device_id=at(*peer), device_id_type=MESH)
    for k in range(owners):
        for h in range(2):
            stage[k, :, h * half:(h + 1) * half] = x_ref[pl.ds(2 * k + h, rows_here, stride=2 * owners), :]
    pl.semaphore_wait(barrier, len(peers))

    def rows_of(owner):
        return pl.ds(pl.multiple_of(owner * rows_here, rows_here), rows_here)

    incoming = []
    for d in range(1, owners):
        copy = pltpu.make_async_remote_copy(
            stage.at[(mine + d) % owners], held.at[rows_of(mine), :], in_send.at[d], in_recv.at[d],
            device_id=at(d), device_id_type=MESH)
        copy.start()
        incoming.append(copy)
    held[rows_of(mine), :] = stage[mine]

    for s in range(steps):
        before = None
        for r in range(rounds):
            forward, backward = orders(plan_ref[s * rounds + r:s * rounds + r + 1, :])
            if r == 0:
                moves[s, r] = forward
                moves_t[s, r] = backward
            else:
                moves[s, r] = dot(before[1], forward).astype(BF16)
                moves_t[s, r] = dot(backward, before[0]).astype(BF16)
            before = forward, backward
        moves[s, rounds] = before[1]

    for copy in incoming:
        copy.wait()

    x = held[...]
    for s in range(steps):
        gram = exact_dot(x.T, x)
        if groups > 1:
            grams[s, group] = gram
            shared = []
            for g in range(1, groups):
                copy = pltpu.make_async_remote_copy(
                    grams.at[s, group], grams.at[s, group], gram_send.at[s, g], gram_recv.at[s, g],
                    device_id=at(0, 0, g), device_id_type=MESH)
                copy.start()
                shared.append(copy)
            for copy in shared:
                copy.wait()
            gram = grams[s, 0]
            for g in range(1, groups):
                gram = gram + grams[s, g]
        rotation = diagonalizer(gram, s, moves, moves_t, rounds)
        if s + 1 < steps:
            bottoms[s] = exact_dot(x, rotation[:, half:])
            copy = pltpu.make_async_remote_copy(
                bottoms.at[s], landed.at[s], mid_sem.at[s, 0], mid_sem.at[s, 1],
                device_id=(me, right), device_id_type=MESH)
            copy.start()
            top = exact_dot(x, rotation[:, :half])
            copy.wait()
            x = jnp.concatenate([top, landed[s]], axis=1)

    ybot[...] = exact_dot(x, rotation[:, half:])
    outgoing = []
    for d in range(owners):
        copy = pltpu.make_async_remote_copy(
            ybot.at[rows_of((mine + d) % owners), :], arrived.at[1, mine], low_send.at[d], low_recv.at[d],
            device_id=at(d, 1), device_id_type=MESH)
        copy.start()
        outgoing.append(copy)
    ytop[...] = exact_dot(x, rotation[:, :half])
    for d in range(1, owners):
        copy = pltpu.make_async_remote_copy(
            ytop.at[rows_of((mine + d) % owners), :], arrived.at[0, mine], top_send.at[d], top_recv.at[d],
            device_id=at(d), device_id_type=MESH)
        copy.start()
        outgoing.append(copy)
    arrived[0, mine] = ytop[rows_of(mine), :]
    for copy in outgoing:
        copy.wait()
    for k in range(owners):
        for h in range(2):
            out_ref[pl.ds(2 * k + h, rows_here, stride=2 * owners), :] = arrived[h, k]


def body(mesh_sizes, matrix, plan):
    rows_here, pair_here, halves, half = matrix.shape
    steps, rounds, width = plan.shape
    rows, cols = mesh_sizes
    owners, groups = pair_here, rows // pair_here
    assert rows % pair_here == 0 and halves == 2 and cols > 1
    sizes = (owners, groups, cols, rows_here, steps, rounds, width)
    dma = pltpu.SemaphoreType.DMA
    rows_all = owners * rows_here
    vmem = pl.BlockSpec(memory_space=pltpu.VMEM)
    out = pl.pallas_call(
        functools.partial(kernel, sizes),
        out_shape=jax.ShapeDtypeStruct((rows_here * pair_here * 2, half), F32),
        in_specs=[vmem, vmem],
        out_specs=vmem,
        scratch_shapes=[
            pltpu.VMEM((owners, rows_here, width), F32),
            pltpu.VMEM((rows_all, width), F32),
            pltpu.VMEM((steps - 1, rows_all, half), F32),
            pltpu.VMEM((steps - 1, rows_all, half), F32),
            pltpu.VMEM((rows_all, half), F32),
            pltpu.VMEM((rows_all, half), F32),
            pltpu.VMEM((2, owners, rows_here, half), F32),
            pltpu.VMEM((steps, rounds + 1, width, width), BF16),
            pltpu.VMEM((steps, rounds, width, width), BF16),
            pltpu.VMEM((steps, groups, width, width) if groups > 1 else (1, 1, 8, 128), F32),
            dma((owners,)), dma((owners,)), dma((steps, 2)), dma((steps, groups)), dma((steps, groups)),
            dma((owners,)), dma((owners,)), dma((owners,)), dma((owners,)),
        ],
        compiler_params=pltpu.CompilerParams(collective_id=0, has_side_effects=True, vmem_limit_bytes=48 << 20),
    )(matrix.reshape(rows_here * pair_here * 2, half), plan.reshape(steps * rounds, width))
    return out.reshape(matrix.shape)


def solution(mesh):
    in_specs = (P("rows", "cols", None, None), P())
    out_specs = P("rows", "cols", None, None)
    sizes = (mesh.shape["rows"], mesh.shape["cols"])
    return jax.shard_map(functools.partial(body, sizes), mesh=mesh, in_specs=in_specs, out_specs=out_specs, check_vma=False)
```

```python
import functools

import jax
import jax.numpy as jnp
from jax import lax
from jax.experimental import pallas as pl
from jax.experimental.pallas import tpu as pltpu
from jax.sharding import PartitionSpec as P

MESH = pl.DeviceIdType.MESH
NN = (((1,), (0,)), ((), ()))
NT = (((1,), (1,)), ((), ()))
F32 = jnp.float32
BF16 = jnp.bfloat16


def dot(a, b, dims=NN, precision=None):
    return lax.dot_general(a, b, dims, precision=precision, preferred_element_type=F32)


def exact_dot(a, b, dims=NN):
    return dot(a, b, dims, lax.Precision.HIGHEST)


def split(a):
    hi = a.astype(BF16)
    rest = a - hi.astype(F32)
    mid = rest.astype(BF16)
    lo = (rest - mid.astype(F32)).astype(BF16)
    return hi, mid, lo


def moved_columns(a, onehot):
    hi, mid, lo = split(a)
    return dot(hi, onehot) + dot(mid, onehot) + dot(lo, onehot)


def moved_transposed(a, onehot_t):
    hi, mid, lo = split(a)
    return dot(onehot_t, hi, NT) + dot(onehot_t, mid, NT) + dot(onehot_t, lo, NT)


def rotated_columns(a, cosine, sine):
    half = a.shape[1] // 2
    left, right = a[:, :half], a[:, half:]
    return jnp.concatenate([cosine * left - sine * right, sine * left + cosine * right], axis=1)


def angles(gram):
    half = gram.shape[0] // 2
    shape = (half, half)
    eye = lax.broadcasted_iota(jnp.int32, shape, 0) == lax.broadcasted_iota(jnp.int32, shape, 1)

    def diagonal(block):
        return jnp.sum(jnp.where(eye, block, 0.0), axis=0, keepdims=True)

    low = diagonal(gram[:half, :half])
    high = diagonal(gram[half:, half:])
    cross = diagonal(gram[:half, half:])
    spread = high - low
    sign = jnp.where(spread >= 0.0, 1.0, -1.0)
    root = jnp.sqrt(spread * spread + 4.0 * cross * cross)
    tangent = sign * 2.0 * cross / (jnp.abs(spread) + root)
    cosine = 1.0 / jnp.sqrt(1.0 + tangent * tangent)
    return cosine, tangent * cosine


def orders(partner):
    width = partner.shape[1]
    shape = (width, width)
    row = lax.broadcasted_iota(jnp.int32, shape, 0)
    col = lax.broadcasted_iota(jnp.int32, shape, 1)
    other = jnp.broadcast_to(partner, shape)
    swap = row == other
    one = jnp.ones(shape, BF16)

    def bits(mask):
        return jnp.where(mask, 1.0, 0.0).astype(BF16)

    swap_b = bits(swap)
    first_row = other > col
    rank_row = dot(bits(first_row), bits(row < col))
    mate_row = dot(rank_row.astype(BF16), swap_b)
    place_row = jnp.where(first_row, rank_row, mate_row + float(width // 2))
    first_col = dot(bits(swap & (col > row)), one) > 0.5
    rank_col = dot(bits(col < row), bits(first_col))
    mate_col = dot(swap_b, rank_col.astype(BF16))
    place_col = jnp.where(first_col, rank_col, mate_col + float(width // 2))
    forward = bits(place_col == col.astype(F32))
    backward = bits(place_row == row.astype(F32))
    return forward, backward


def diagonalizer(gram, step, moves, moves_t, rounds, want_rotation):
    rotation = None
    cosines, sines = [], []
    for r in range(rounds):
        move = moves[step, r]
        if r == 0:
            turned = moved_transposed(gram, moves_t[step, r])
            gram = moved_columns(turned, move)
        else:
            turned = moved_transposed(rotated_columns(gram, cosines[-1], sines[-1]), moves_t[step, r])
            gram = moved_columns(rotated_columns(turned, cosines[-1], sines[-1]), move)
        cosine, sine = angles(gram)
        cosines.append(cosine)
        sines.append(sine)
        if want_rotation:
            rotation = move.astype(F32) if r == 0 else moved_columns(rotation, move)
            rotation = rotated_columns(rotation, cosine, sine)
    if want_rotation:
        rotation = moved_columns(rotation, moves[step, rounds])
    return jnp.concatenate(cosines + sines, axis=0), rotation


def turn_rows(x, turns, step, moves, rounds):
    pairs, rows, width = x.shape
    half = width // 2
    x = x.reshape(pairs * rows, width)
    for r in range(rounds):
        x = moved_columns(x, moves[step, r]).reshape(pairs, rows, width)
        cosine, sine = turns[:, r:r + 1, :], turns[:, rounds + r:rounds + r + 1, :]
        left, right = x[:, :, :half], x[:, :, half:]
        x = jnp.concatenate([cosine * left - sine * right, sine * left + cosine * right], axis=2)
        x = x.reshape(pairs * rows, width)
    return moved_columns(x, moves[step, rounds]).reshape(pairs, rows, width)


def kernel(sizes, x_ref, plan_ref, out_ref, stage, held, bottoms, landed, row_tops, row_low, row_landed, turns,
           moves, moves_t, grams, in_send, in_recv, mid_sem, gram_send, gram_recv, turn_send, turn_recv,
           row_send, row_recv):
    owners, groups, cols, rows_here, steps, rounds, width = sizes
    half = width // 2
    me = lax.axis_index("rows")
    col = lax.axis_index("cols")
    group, mine = me // owners, me % owners
    right = (col + 1) % cols

    def at(owner_shift, col_shift=0, group_shift=0):
        row = ((group + group_shift) % groups) * owners + (mine + owner_shift) % owners
        return row, (col + col_shift) % cols

    peers = {(o, 0, 0) for o in range(owners)} | {(0, c, 0) for c in (1, cols - 1)} | {(0, 0, g) for g in range(groups)}
    peers = sorted(peers - {(0, 0, 0)})
    barrier = pltpu.get_barrier_semaphore()
    for peer in peers:
        pl.semaphore_signal(barrier, inc=1, device_id=at(*peer), device_id_type=MESH)
    for k in range(owners):
        for h in range(2):
            stage[k, :, h * half:(h + 1) * half] = x_ref[pl.ds(2 * k + h, rows_here, stride=2 * owners), :]
    pl.semaphore_wait(barrier, len(peers))

    def rows_of(owner):
        return pl.ds(pl.multiple_of(owner * rows_here, rows_here), rows_here)

    incoming = []
    for d in range(1, owners):
        copy = pltpu.make_async_remote_copy(
            stage.at[(mine + d) % owners], held.at[rows_of(mine), :], in_send.at[d], in_recv.at[d],
            device_id=at(d), device_id_type=MESH)
        copy.start()
        incoming.append(copy)
    held[rows_of(mine), :] = stage[mine]

    for s in range(steps):
        before = None
        for r in range(rounds):
            forward, backward = orders(plan_ref[s, r:r + 1, :])
            if r == 0:
                moves[s, r] = forward
                moves_t[s, r] = backward
            else:
                moves[s, r] = dot(before[1], forward).astype(BF16)
                moves_t[s, r] = dot(backward, before[0]).astype(BF16)
            before = forward, backward
        moves[s, rounds] = before[1]

    for copy in incoming:
        copy.wait()

    x = held[...]
    chunks = 2 if owners % 2 == 0 else 1
    passing = []
    for s in range(steps):
        gram = exact_dot(x.T, x)
        if groups > 1:
            grams[s, group] = gram
            shared = []
            for g in range(1, groups):
                copy = pltpu.make_async_remote_copy(
                    grams.at[s, group], grams.at[s, group], gram_send.at[s, g], gram_recv.at[s, g],
                    device_id=at(0, 0, g), device_id_type=MESH)
                copy.start()
                shared.append(copy)
            for copy in shared:
                copy.wait()
            gram = grams[s, 0]
            for g in range(1, groups):
                gram = gram + grams[s, g]
        last = s + 1 == steps
        angle, rotation = diagonalizer(gram, s, moves, moves_t, rounds, not last)
        turns[s, mine] = angle
        told = []
        for d in range(1, owners):
            copy = pltpu.make_async_remote_copy(
                turns.at[s, mine], turns.at[s, mine], turn_send.at[s, d], turn_recv.at[s, d],
                device_id=at(d), device_id_type=MESH)
            copy.start()
            told.append(copy)
        if not last:
            bottoms[s] = exact_dot(x, rotation[:, half:])
            crossing = pltpu.make_async_remote_copy(
                bottoms.at[s], landed.at[s], mid_sem.at[s, 0], mid_sem.at[s, 1],
                device_id=(me, right), device_id_type=MESH)
            crossing.start()
            top = exact_dot(x, rotation[:, :half])
        if s > 0:
            for copy in passing:
                copy.wait()
        for copy in told:
            copy.wait()
        passing = []
        size = owners // chunks
        for q in range(chunks):
            part = slice(q * size, (q + 1) * size)
            if s == 0:
                rows = stage[part]
            else:
                rows = jnp.concatenate([row_tops[s - 1, part], row_landed[s - 1, part]], axis=2)
            rows = turn_rows(rows, turns[s, part], s, moves, rounds)
            row_low[s, part] = rows[:, :, half:]
            copy = pltpu.make_async_remote_copy(
                row_low.at[s, part], row_landed.at[s, part], row_send.at[s, q], row_recv.at[s, q],
                device_id=(me, right), device_id_type=MESH)
            copy.start()
            passing.append(copy)
            if last:
                for k in range(size):
                    out_ref[pl.ds(2 * (q * size + k), rows_here, stride=2 * owners), :] = rows[k, :, :half]
            else:
                row_tops[s, part] = rows[:, :, :half]
        if not last:
            crossing.wait()
            x = jnp.concatenate([top, landed[s]], axis=1)

    for q in range(chunks):
        passing[q].wait()
        for k in range(q * size, (q + 1) * size):
            out_ref[pl.ds(2 * k + 1, rows_here, stride=2 * owners), :] = row_landed[steps - 1, k]


def body(mesh_sizes, matrix, plan):
    rows_here, pair_here, halves, half = matrix.shape
    steps, rounds, width = plan.shape
    rows, cols = mesh_sizes
    owners, groups = pair_here, rows // pair_here
    assert rows % pair_here == 0 and halves == 2 and cols > 1
    sizes = (owners, groups, cols, rows_here, steps, rounds, width)
    dma = pltpu.SemaphoreType.DMA
    rows_all = owners * rows_here
    vmem = pl.BlockSpec(memory_space=pltpu.VMEM)
    out = pl.pallas_call(
        functools.partial(kernel, sizes),
        out_shape=jax.ShapeDtypeStruct((rows_here * pair_here * 2, half), F32),
        in_specs=[vmem, vmem],
        out_specs=vmem,
        scratch_shapes=[
            pltpu.VMEM((owners, rows_here, width), F32),
            pltpu.VMEM((rows_all, width), F32),
            pltpu.VMEM((steps - 1, rows_all, half), F32),
            pltpu.VMEM((steps - 1, rows_all, half), F32),
            pltpu.VMEM((steps, owners, rows_here, half), F32),
            pltpu.VMEM((steps, owners, rows_here, half), F32),
            pltpu.VMEM((steps, owners, rows_here, half), F32),
            pltpu.VMEM((steps, owners, 2 * rounds, half), F32),
            pltpu.VMEM((steps, rounds + 1, width, width), BF16),
            pltpu.VMEM((steps, rounds, width, width), BF16),
            pltpu.VMEM((steps, groups, width, width) if groups > 1 else (1, 1, 8, 128), F32),
            dma((owners,)), dma((owners,)), dma((steps, 2)), dma((steps, groups)), dma((steps, groups)),
            dma((steps, owners)), dma((steps, owners)), dma((steps, 2)), dma((steps, 2)),
        ],
        compiler_params=pltpu.CompilerParams(collective_id=0, has_side_effects=True, vmem_limit_bytes=48 << 20),
    )(matrix.reshape(rows_here * pair_here * 2, half), plan)
    return out.reshape(matrix.shape)


def solution(mesh):
    in_specs = (P("rows", "cols", None, None), P())
    out_specs = P("rows", "cols", None, None)
    sizes = (mesh.shape["rows"], mesh.shape["cols"])
    return jax.shard_map(functools.partial(body, sizes), mesh=mesh, in_specs=in_specs, out_specs=out_specs, check_vma=False)
```

```python
import functools

import jax
import jax.numpy as jnp
from jax import lax
from jax.experimental import pallas as pl
from jax.experimental.pallas import tpu as pltpu
from jax.sharding import PartitionSpec as P

MESH = pl.DeviceIdType.MESH
NN = (((1,), (0,)), ((), ()))
NT = (((1,), (1,)), ((), ()))
F32 = jnp.float32
BF16 = jnp.bfloat16


def dot(a, b, dims=NN, precision=None):
    return lax.dot_general(a, b, dims, precision=precision, preferred_element_type=F32)


def exact_dot(a, b, dims=NN):
    return dot(a, b, dims, lax.Precision.HIGHEST)


def split(a):
    hi = a.astype(BF16)
    rest = a - hi.astype(F32)
    mid = rest.astype(BF16)
    lo = (rest - mid.astype(F32)).astype(BF16)
    return hi, mid, lo


def moved_columns(a, onehot):
    hi, mid, lo = split(a)
    return dot(hi, onehot) + dot(mid, onehot) + dot(lo, onehot)


def moved_transposed(a, onehot_t):
    hi, mid, lo = split(a)
    return dot(onehot_t, hi, NT) + dot(onehot_t, mid, NT) + dot(onehot_t, lo, NT)


def rotated_columns(a, cosine, sine):
    half = a.shape[1] // 2
    left, right = a[:, :half], a[:, half:]
    return jnp.concatenate([cosine * left - sine * right, sine * left + cosine * right], axis=1)


def angles(gram):
    half = gram.shape[0] // 2
    shape = (half, half)
    eye = lax.broadcasted_iota(jnp.int32, shape, 0) == lax.broadcasted_iota(jnp.int32, shape, 1)

    def diagonal(block):
        return jnp.sum(jnp.where(eye, block, 0.0), axis=0, keepdims=True)

    low = diagonal(gram[:half, :half])
    high = diagonal(gram[half:, half:])
    cross = diagonal(gram[:half, half:])
    spread = high - low
    sign = jnp.where(spread >= 0.0, 1.0, -1.0)
    root = jnp.sqrt(spread * spread + 4.0 * cross * cross)
    tangent = sign * 2.0 * cross / (jnp.abs(spread) + root)
    cosine = 1.0 / jnp.sqrt(1.0 + tangent * tangent)
    return cosine, tangent * cosine


def orders(partner):
    width = partner.shape[1]
    shape = (width, width)
    row = lax.broadcasted_iota(jnp.int32, shape, 0)
    col = lax.broadcasted_iota(jnp.int32, shape, 1)
    other = jnp.broadcast_to(partner, shape)
    swap = row == other
    one = jnp.ones(shape, BF16)

    def bits(mask):
        return jnp.where(mask, 1.0, 0.0).astype(BF16)

    swap_b = bits(swap)
    first_row = other > col
    rank_row = dot(bits(first_row), bits(row < col))
    mate_row = dot(rank_row.astype(BF16), swap_b)
    place_row = jnp.where(first_row, rank_row, mate_row + float(width // 2))
    first_col = dot(bits(swap & (col > row)), one) > 0.5
    rank_col = dot(bits(col < row), bits(first_col))
    mate_col = dot(swap_b, rank_col.astype(BF16))
    place_col = jnp.where(first_col, rank_col, mate_col + float(width // 2))
    forward = bits(place_col == col.astype(F32))
    backward = bits(place_row == row.astype(F32))
    return forward, backward


def diagonalizer(gram, step, moves, moves_t, rounds, want_rotation):
    rotation = None
    cosines, sines = [], []
    for r in range(rounds):
        move = moves[step, r]
        if r == 0:
            turned = moved_transposed(gram, moves_t[step, r])
            gram = moved_columns(turned, move)
        else:
            turned = moved_transposed(rotated_columns(gram, cosines[-1], sines[-1]), moves_t[step, r])
            gram = moved_columns(rotated_columns(turned, cosines[-1], sines[-1]), move)
        cosine, sine = angles(gram)
        cosines.append(cosine)
        sines.append(sine)
        if want_rotation:
            rotation = move.astype(F32) if r == 0 else moved_columns(rotation, move)
            rotation = rotated_columns(rotation, cosine, sine)
    if want_rotation:
        rotation = moved_columns(rotation, moves[step, rounds])
    return jnp.concatenate(cosines + sines, axis=0), rotation


def turn_rows(x, turns, step, moves, rounds):
    pairs, rows, width = x.shape
    half = width // 2
    x = x.reshape(pairs * rows, width)
    for r in range(rounds):
        x = moved_columns(x, moves[step, r]).reshape(pairs, rows, width)
        cosine, sine = turns[:, r:r + 1, :], turns[:, rounds + r:rounds + r + 1, :]
        left, right = x[:, :, :half], x[:, :, half:]
        x = jnp.concatenate([cosine * left - sine * right, sine * left + cosine * right], axis=2)
        x = x.reshape(pairs * rows, width)
    return moved_columns(x, moves[step, rounds]).reshape(pairs, rows, width)


def kernel(sizes, x_ref, plan_ref, out_ref, stage, held, bottoms, landed, row_tops, row_low, row_landed, turns,
           moves, moves_t, grams, in_send, in_recv, mid_sem, gram_send, gram_recv, turn_send, turn_recv,
           row_send, row_recv):
    owners, groups, cols, rows_here, steps, rounds, width = sizes
    half = width // 2
    me = lax.axis_index("rows")
    col = lax.axis_index("cols")
    group, mine = me // owners, me % owners
    right = (col + 1) % cols

    def at(owner_shift, col_shift=0, group_shift=0):
        row = ((group + group_shift) % groups) * owners + (mine + owner_shift) % owners
        return row, (col + col_shift) % cols

    peers = {(o, 0, 0) for o in range(owners)} | {(0, c, 0) for c in (1, cols - 1)} | {(0, 0, g) for g in range(groups)}
    peers = sorted(peers - {(0, 0, 0)})
    barrier = pltpu.get_barrier_semaphore()
    for peer in peers:
        pl.semaphore_signal(barrier, inc=1, device_id=at(*peer), device_id_type=MESH)
    for k in range(owners):
        for h in range(2):
            stage[k, :, h * half:(h + 1) * half] = x_ref[pl.ds(2 * k + h, rows_here, stride=2 * owners), :]
    pl.semaphore_wait(barrier, len(peers))

    def rows_of(owner):
        return pl.ds(pl.multiple_of(owner * rows_here, rows_here), rows_here)

    incoming = []
    for d in sorted(range(1, owners), key=lambda d: -min(d, owners - d)):
        copy = pltpu.make_async_remote_copy(
            stage.at[(mine + d) % owners], held.at[rows_of(mine), :], in_send.at[d], in_recv.at[d],
            device_id=at(d), device_id_type=MESH)
        copy.start()
        incoming.append(copy)
    held[rows_of(mine), :] = stage[mine]

    for s in range(steps):
        before = None
        for r in range(rounds):
            forward, backward = orders(plan_ref[s, r:r + 1, :])
            if r == 0:
                moves[s, r] = forward
                moves_t[s, r] = backward
            else:
                moves[s, r] = dot(before[1], forward).astype(BF16)
                moves_t[s, r] = dot(backward, before[0]).astype(BF16)
            before = forward, backward
        moves[s, rounds] = before[1]

    for copy in incoming:
        copy.wait()

    x = held[...]
    chunks = 2 if owners % 2 == 0 else 1
    passing = []
    for s in range(steps):
        gram = exact_dot(x.T, x)
        if groups > 1:
            grams[s, group] = gram
            shared = []
            for g in range(1, groups):
                copy = pltpu.make_async_remote_copy(
                    grams.at[s, group], grams.at[s, group], gram_send.at[s, g], gram_recv.at[s, g],
                    device_id=at(0, 0, g), device_id_type=MESH)
                copy.start()
                shared.append(copy)
            for copy in shared:
                copy.wait()
            gram = grams[s, 0]
            for g in range(1, groups):
                gram = gram + grams[s, g]
        last = s + 1 == steps
        angle, rotation = diagonalizer(gram, s, moves, moves_t, rounds, not last)
        turns[s, mine] = angle
        told = []
        for d in range(1, owners):
            copy = pltpu.make_async_remote_copy(
                turns.at[s, mine], turns.at[s, mine], turn_send.at[s, d], turn_recv.at[s, d],
                device_id=at(d), device_id_type=MESH)
            copy.start()
            told.append(copy)
        if not last:
            bottoms[s] = exact_dot(x, rotation[:, half:])
            crossing = pltpu.make_async_remote_copy(
                bottoms.at[s], landed.at[s], mid_sem.at[s, 0], mid_sem.at[s, 1],
                device_id=(me, right), device_id_type=MESH)
            crossing.start()
            top = exact_dot(x, rotation[:, :half])
        if s > 0:
            for copy in passing:
                copy.wait()
        for copy in told:
            copy.wait()
        passing = []
        size = owners // chunks
        for q in range(chunks):
            part = slice(q * size, (q + 1) * size)
            if s == 0:
                rows = stage[part]
            else:
                rows = jnp.concatenate([row_tops[s - 1, part], row_landed[s - 1, part]], axis=2)
            rows = turn_rows(rows, turns[s, part], s, moves, rounds)
            row_low[s, part] = rows[:, :, half:]
            copy = pltpu.make_async_remote_copy(
                row_low.at[s, part], row_landed.at[s, part], row_send.at[s, q], row_recv.at[s, q],
                device_id=(me, right), device_id_type=MESH)
            copy.start()
            passing.append(copy)
            if last:
                for k in range(size):
                    out_ref[pl.ds(2 * (q * size + k), rows_here, stride=2 * owners), :] = rows[k, :, :half]
            else:
                row_tops[s, part] = rows[:, :, :half]
        if not last:
            crossing.wait()
            x = jnp.concatenate([top, landed[s]], axis=1)

    for q in range(chunks):
        passing[q].wait()
        for k in range(q * size, (q + 1) * size):
            out_ref[pl.ds(2 * k + 1, rows_here, stride=2 * owners), :] = row_landed[steps - 1, k]


def body(mesh_sizes, matrix, plan):
    rows_here, pair_here, halves, half = matrix.shape
    steps, rounds, width = plan.shape
    rows, cols = mesh_sizes
    owners, groups = pair_here, rows // pair_here
    assert rows % pair_here == 0 and halves == 2 and cols > 1
    sizes = (owners, groups, cols, rows_here, steps, rounds, width)
    dma = pltpu.SemaphoreType.DMA
    rows_all = owners * rows_here
    vmem = pl.BlockSpec(memory_space=pltpu.VMEM)
    out = pl.pallas_call(
        functools.partial(kernel, sizes),
        out_shape=jax.ShapeDtypeStruct((rows_here * pair_here * 2, half), F32),
        in_specs=[vmem, vmem],
        out_specs=vmem,
        scratch_shapes=[
            pltpu.VMEM((owners, rows_here, width), F32),
            pltpu.VMEM((rows_all, width), F32),
            pltpu.VMEM((steps - 1, rows_all, half), F32),
            pltpu.VMEM((steps - 1, rows_all, half), F32),
            pltpu.VMEM((steps, owners, rows_here, half), F32),
            pltpu.VMEM((steps, owners, rows_here, half), F32),
            pltpu.VMEM((steps, owners, rows_here, half), F32),
            pltpu.VMEM((steps, owners, 2 * rounds, half), F32),
            pltpu.VMEM((steps, rounds + 1, width, width), BF16),
            pltpu.VMEM((steps, rounds, width, width), BF16),
            pltpu.VMEM((steps, groups, width, width) if groups > 1 else (1, 1, 8, 128), F32),
            dma((owners,)), dma((owners,)), dma((steps, 2)), dma((steps, groups)), dma((steps, groups)),
            dma((steps, owners)), dma((steps, owners)), dma((steps, 2)), dma((steps, 2)),
        ],
        compiler_params=pltpu.CompilerParams(collective_id=0, has_side_effects=True, vmem_limit_bytes=48 << 20),
    )(matrix.reshape(rows_here * pair_here * 2, half), plan)
    return out.reshape(matrix.shape)


def solution(mesh):
    in_specs = (P("rows", "cols", None, None), P())
    out_specs = P("rows", "cols", None, None)
    sizes = (mesh.shape["rows"], mesh.shape["cols"])
    return jax.shard_map(functools.partial(body, sizes), mesh=mesh, in_specs=in_specs, out_specs=out_specs, check_vma=False)
```

```python
import functools

import jax
import jax.numpy as jnp
from jax import lax
from jax.experimental import pallas as pl
from jax.experimental.pallas import tpu as pltpu
from jax.sharding import PartitionSpec as P

MESH = pl.DeviceIdType.MESH
NN = (((1,), (0,)), ((), ()))
NT = (((1,), (1,)), ((), ()))
F32 = jnp.float32
BF16 = jnp.bfloat16


def dot(a, b, dims=NN, precision=None):
    return lax.dot_general(a, b, dims, precision=precision, preferred_element_type=F32)


def exact_dot(a, b, dims=NN):
    return dot(a, b, dims, lax.Precision.HIGHEST)


def split(a):
    hi = a.astype(BF16)
    rest = a - hi.astype(F32)
    mid = rest.astype(BF16)
    lo = (rest - mid.astype(F32)).astype(BF16)
    return hi, mid, lo


def moved_columns(a, onehot):
    hi, mid, lo = split(a)
    return dot(hi, onehot) + dot(mid, onehot) + dot(lo, onehot)


def moved_transposed(a, onehot_t):
    hi, mid, lo = split(a)
    return dot(onehot_t, hi, NT) + dot(onehot_t, mid, NT) + dot(onehot_t, lo, NT)


def rotated_columns(a, cosine, sine):
    half = a.shape[1] // 2
    left, right = a[:, :half], a[:, half:]
    return jnp.concatenate([cosine * left - sine * right, sine * left + cosine * right], axis=1)


def angles(gram):
    half = gram.shape[0] // 2
    shape = (half, half)
    eye = lax.broadcasted_iota(jnp.int32, shape, 0) == lax.broadcasted_iota(jnp.int32, shape, 1)

    def diagonal(block):
        return jnp.sum(jnp.where(eye, block, 0.0), axis=0, keepdims=True)

    low = diagonal(gram[:half, :half])
    high = diagonal(gram[half:, half:])
    cross = diagonal(gram[:half, half:])
    spread = high - low
    sign = jnp.where(spread >= 0.0, 1.0, -1.0)
    root = jnp.sqrt(spread * spread + 4.0 * cross * cross)
    tangent = sign * 2.0 * cross / (jnp.abs(spread) + root)
    cosine = 1.0 / jnp.sqrt(1.0 + tangent * tangent)
    return cosine, tangent * cosine


def orders(partner):
    width = partner.shape[1]
    shape = (width, width)
    row = lax.broadcasted_iota(jnp.int32, shape, 0)
    col = lax.broadcasted_iota(jnp.int32, shape, 1)
    other = jnp.broadcast_to(partner, shape)
    swap = row == other
    one = jnp.ones(shape, BF16)

    def bits(mask):
        return jnp.where(mask, 1.0, 0.0).astype(BF16)

    swap_b = bits(swap)
    first_row = other > col
    rank_row = dot(bits(first_row), bits(row < col))
    mate_row = dot(rank_row.astype(BF16), swap_b)
    place_row = jnp.where(first_row, rank_row, mate_row + float(width // 2))
    first_col = dot(bits(swap & (col > row)), one) > 0.5
    rank_col = dot(bits(col < row), bits(first_col))
    mate_col = dot(swap_b, rank_col.astype(BF16))
    place_col = jnp.where(first_col, rank_col, mate_col + float(width // 2))
    forward = bits(place_col == col.astype(F32))
    backward = bits(place_row == row.astype(F32))
    return forward, backward


def diagonalizer(gram, step, moves, moves_t, rounds, want_rotation):
    rotation = None
    cosines, sines = [], []
    for r in range(rounds):
        move = moves[step, r]
        if r == 0:
            turned = moved_transposed(gram, moves_t[step, r])
            gram = moved_columns(turned, move)
        else:
            turned = moved_transposed(rotated_columns(gram, cosines[-1], sines[-1]), moves_t[step, r])
            gram = moved_columns(rotated_columns(turned, cosines[-1], sines[-1]), move)
        cosine, sine = angles(gram)
        cosines.append(cosine)
        sines.append(sine)
        if want_rotation:
            rotation = move.astype(F32) if r == 0 else moved_columns(rotation, move)
            rotation = rotated_columns(rotation, cosine, sine)
    if want_rotation:
        rotation = moved_columns(rotation, moves[step, rounds])
    return jnp.concatenate(cosines + sines, axis=0), rotation


def turn_rows(x, turns, step, moves, rounds):
    pairs, rows, width = x.shape
    half = width // 2
    for r in range(rounds):
        if r > 0:
            x = moved_columns(x, moves[step, r]).reshape(pairs, rows, width)
        cosine, sine = turns[:, r:r + 1, :], turns[:, rounds + r:rounds + r + 1, :]
        left, right = x[:, :, :half], x[:, :, half:]
        x = jnp.concatenate([cosine * left - sine * right, sine * left + cosine * right], axis=2)
        x = x.reshape(pairs * rows, width)
    return moved_columns(x, moves[step, rounds]).reshape(pairs, rows, width)


def kernel(sizes, x_ref, plan_ref, out_ref, stage, held, bottoms, landed, row_tops, row_low, row_landed, turns,
           moves, moves_t, grams, in_send, in_recv, mid_sem, gram_send, gram_recv, turn_send, turn_recv,
           row_send, row_recv):
    owners, groups, cols, rows_here, steps, rounds, width = sizes
    half = width // 2
    me = lax.axis_index("rows")
    col = lax.axis_index("cols")
    group, mine = me // owners, me % owners
    right = (col + 1) % cols

    def at(owner_shift, col_shift=0, group_shift=0):
        row = ((group + group_shift) % groups) * owners + (mine + owner_shift) % owners
        return row, (col + col_shift) % cols

    peers = {(o, 0, 0) for o in range(owners)} | {(0, c, 0) for c in (1, cols - 1)} | {(0, 0, g) for g in range(groups)}
    peers = sorted(peers - {(0, 0, 0)})
    barrier = pltpu.get_barrier_semaphore()
    for peer in peers:
        pl.semaphore_signal(barrier, inc=1, device_id=at(*peer), device_id_type=MESH)
    for k in range(owners):
        for h in range(2):
            stage[k, :, h * half:(h + 1) * half] = x_ref[pl.ds(2 * k + h, rows_here, stride=2 * owners), :]
    pl.semaphore_wait(barrier, len(peers))

    def rows_of(owner):
        return pl.ds(pl.multiple_of(owner * rows_here, rows_here), rows_here)

    incoming = []
    for d in range(1, owners):
        copy = pltpu.make_async_remote_copy(
            stage.at[(mine + d) % owners], held.at[rows_of(mine), :], in_send.at[d], in_recv.at[d],
            device_id=at(d), device_id_type=MESH)
        copy.start()
        incoming.append(copy)
    held[rows_of(mine), :] = stage[mine]

    for s in range(steps):
        before = None
        for r in range(rounds):
            forward, backward = orders(plan_ref[s, r:r + 1, :])
            if r == 0:
                moves[s, r] = forward
                moves_t[s, r] = backward
            else:
                moves[s, r] = dot(before[1], forward).astype(BF16)
                moves_t[s, r] = dot(backward, before[0]).astype(BF16)
            before = forward, backward
        moves[s, rounds] = before[1]

    for copy in incoming:
        copy.wait()

    x = held[...]
    chunks = 2 if owners % 2 == 0 else 1
    passing = []
    for s in range(steps):
        gram = exact_dot(x.T, x)
        if groups > 1:
            grams[s, group] = gram
            shared = []
            for g in range(1, groups):
                copy = pltpu.make_async_remote_copy(
                    grams.at[s, group], grams.at[s, group], gram_send.at[s, g], gram_recv.at[s, g],
                    device_id=at(0, 0, g), device_id_type=MESH)
                copy.start()
                shared.append(copy)
            for copy in shared:
                copy.wait()
            gram = grams[s, 0]
            for g in range(1, groups):
                gram = gram + grams[s, g]
        last = s + 1 == steps
        angle, rotation = diagonalizer(gram, s, moves, moves_t, rounds, not last)
        turns[s, mine] = angle
        told = []
        for d in range(1, owners):
            copy = pltpu.make_async_remote_copy(
                turns.at[s, mine], turns.at[s, mine], turn_send.at[s, d], turn_recv.at[s, d],
                device_id=at(d), device_id_type=MESH)
            copy.start()
            told.append(copy)
        if not last:
            bottoms[s] = exact_dot(x, rotation[:, half:])
            crossing = pltpu.make_async_remote_copy(
                bottoms.at[s], landed.at[s], mid_sem.at[s, 0], mid_sem.at[s, 1],
                device_id=(me, right), device_id_type=MESH)
            crossing.start()
            top = exact_dot(x, rotation[:, :half])
        if s > 0:
            for copy in passing:
                copy.wait()
        size = owners // chunks
        ordered = []
        for q in range(chunks):
            part = slice(q * size, (q + 1) * size)
            if s == 0:
                rows = stage[part]
            else:
                rows = jnp.concatenate([row_tops[s - 1, part], row_landed[s - 1, part]], axis=2)
            flat = moved_columns(rows.reshape(size * rows_here, width), moves[s, 0])
            ordered.append(flat.reshape(size, rows_here, width))
        for copy in told:
            copy.wait()
        passing = []
        for q in range(chunks):
            part = slice(q * size, (q + 1) * size)
            rows = turn_rows(ordered[q], turns[s, part], s, moves, rounds)
            row_low[s, part] = rows[:, :, half:]
            copy = pltpu.make_async_remote_copy(
                row_low.at[s, part], row_landed.at[s, part], row_send.at[s, q], row_recv.at[s, q],
                device_id=(me, right), device_id_type=MESH)
            copy.start()
            passing.append(copy)
            if last:
                for k in range(size):
                    out_ref[pl.ds(2 * (q * size + k), rows_here, stride=2 * owners), :] = rows[k, :, :half]
            else:
                row_tops[s, part] = rows[:, :, :half]
        if not last:
            crossing.wait()
            x = jnp.concatenate([top, landed[s]], axis=1)

    for q in range(chunks):
        passing[q].wait()
        for k in range(q * size, (q + 1) * size):
            out_ref[pl.ds(2 * k + 1, rows_here, stride=2 * owners), :] = row_landed[steps - 1, k]


def body(mesh_sizes, matrix, plan):
    rows_here, pair_here, halves, half = matrix.shape
    steps, rounds, width = plan.shape
    rows, cols = mesh_sizes
    owners, groups = pair_here, rows // pair_here
    assert rows % pair_here == 0 and halves == 2 and cols > 1
    sizes = (owners, groups, cols, rows_here, steps, rounds, width)
    dma = pltpu.SemaphoreType.DMA
    rows_all = owners * rows_here
    vmem = pl.BlockSpec(memory_space=pltpu.VMEM)
    out = pl.pallas_call(
        functools.partial(kernel, sizes),
        out_shape=jax.ShapeDtypeStruct((rows_here * pair_here * 2, half), F32),
        in_specs=[vmem, vmem],
        out_specs=vmem,
        scratch_shapes=[
            pltpu.VMEM((owners, rows_here, width), F32),
            pltpu.VMEM((rows_all, width), F32),
            pltpu.VMEM((steps - 1, rows_all, half), F32),
            pltpu.VMEM((steps - 1, rows_all, half), F32),
            pltpu.VMEM((steps, owners, rows_here, half), F32),
            pltpu.VMEM((steps, owners, rows_here, half), F32),
            pltpu.VMEM((steps, owners, rows_here, half), F32),
            pltpu.VMEM((steps, owners, 2 * rounds, half), F32),
            pltpu.VMEM((steps, rounds + 1, width, width), BF16),
            pltpu.VMEM((steps, rounds, width, width), BF16),
            pltpu.VMEM((steps, groups, width, width) if groups > 1 else (1, 1, 8, 128), F32),
            dma((owners,)), dma((owners,)), dma((steps, 2)), dma((steps, groups)), dma((steps, groups)),
            dma((steps, owners)), dma((steps, owners)), dma((steps, 2)), dma((steps, 2)),
        ],
        compiler_params=pltpu.CompilerParams(collective_id=0, has_side_effects=True, vmem_limit_bytes=48 << 20),
    )(matrix.reshape(rows_here * pair_here * 2, half), plan)
    return out.reshape(matrix.shape)


def solution(mesh):
    in_specs = (P("rows", "cols", None, None), P())
    out_specs = P("rows", "cols", None, None)
    sizes = (mesh.shape["rows"], mesh.shape["cols"])
    return jax.shard_map(functools.partial(body, sizes), mesh=mesh, in_specs=in_specs, out_specs=out_specs, check_vma=False)
```
